32 devices in a mesh: facet: 8 (over y, x, core), sub: 4 (over z).
Axes of the slice: x: 2, y: 2, z: 4, core: 2. Of those that a mesh axis runs over, the one named last changes fastest.
Arguments:
- model_image: float32 [8, 128, 8192], P('facet'), may hold values from -6 to 6
- step_sizes: float32 [2], replicated, may hold values from 0.3 to 1
- facet_offsets: int32 [2, 8], replicated, may hold values from 0 to 57344
- col_offsets: int32 [4], P('sub'), may hold values from 0 to 65280
- row_offsets: int32 [4, 8], P('sub'), may hold values from 0 to 65280
- counts: int32 [4, 8], P('sub'), may hold values from 1024 to 4096, as said below
- vis_uv: int32 [2, 4, 8, 4096], P(None, 'sub', 'facet'), may hold values from 32 to 2015
- vis_obs: bfloat16 [2, 4, 8, 4096], P(None, 'sub', 'facet'), may hold values from -6 to 6
- vis_weight: bfloat16 [4, 8, 4096], P('sub', 'facet'), may hold values from 0.25 to 4
Outputs:
- updated_image: float32 [8, 128, 8192], P('facet')
- residual_vis: float32 [2, 4, 8, 4096], P(None, 'sub', 'facet')
The draws below stay inside these ranges and needn't reach their ends.
Inputs may be any that keep to these rules, and one draw needn't show every extreme that they name: The visibilities of a subgrid fill its first counts slots; every draw has a subgrid with exactly 4096 visibilities and one with exactly 1024.
All inputs are finite; a program needn't handle non-finite values.
Results may differ from the reference program's by a relative error of at most 0.017.
Values may be sent and summed in bfloat16 or wider, within the bound.
A program may use at most 64 MiB of HBM per device.

```python
import math
import jax
import jax.numpy as jnp
from jax import lax

NIMG = 65536
FW = 8192
FROWS = 128
SGW = 256
VCAP = 4096
VMIN = 1024
VB = 512
OS = 8
KSUP = 4
ITERS = 2
FACETS = 8
NCOL = 4
NROWSG = 8


def draw_counts(key, part):
    subgrid_total = NCOL * NROWSG
    draws_raw = jax.random.randint(jax.random.fold_in(key, 11), (subgrid_total,), 0, 1025, dtype=jnp.int32)
    cubed_raw = draws_raw * draws_raw // 1024 * draws_raw // 1024
    values = VMIN + cubed_raw * (VCAP - VMIN) // 1024
    top_slot = jax.random.randint(jax.random.fold_in(key, 12), (), 0, subgrid_total, dtype=jnp.int32)
    low_shift = jax.random.randint(jax.random.fold_in(key, 13), (), 1, subgrid_total, dtype=jnp.int32)
    low_slot = (top_slot + low_shift) % subgrid_total
    slot_ids = jnp.arange(subgrid_total, dtype=jnp.int32)
    values = jnp.where(slot_ids == top_slot, VCAP, values)
    values = jnp.where(slot_ids == low_slot, VMIN, values)
    return values.reshape(NCOL, NROWSG).astype(jnp.int32)


def plant(array, key, low, top_value):
    longest = array.shape.index(max(array.shape))
    spots = []
    for shift in (0, 1):
        where = [jax.random.randint(jax.random.fold_in(key, axis), (), 0, length) for axis, length in enumerate(array.shape)]
        where[longest] = (where[longest] + shift) % array.shape[longest]
        spots.append(tuple(where))
    return array.at[spots[0]].set(low).at[spots[1]].set(top_value)


def shard_levels(key, extent, pieces, smallest, high):
    def one(axis_at, parts):
        steps = jax.random.uniform(jax.random.fold_in(jax.random.fold_in(key, 6), axis_at), (parts,), jnp.float32, smallest / len(pieces), high / len(pieces))
        return jnp.repeat(jnp.exp(steps), extent[axis_at] // parts).reshape((-1,) + (1,) * (len(extent) - axis_at - 1))

    level = one(*pieces[0])
    for cut in pieces[1:]:
        level = level * one(*cut)
    return level


def bell_draw(rng, shape, spread, limit, pieces=(), kind=jnp.bfloat16):
    array = spread * jax.random.normal(rng, shape, jnp.float32)
    if pieces:
        array = array * shard_levels(rng, shape, pieces, -0.22, 0.18)
    return jnp.clip(array, -limit, limit).astype(kind)


def setup_inputs(seed: int = 0) -> dict:
    key_of = jax.random.split(jax.random.key(seed), 10)
    model_image = bell_draw(key_of[0], (FACETS, FROWS, FW), 1.0, 6.0, ((0, 8),), jnp.float32)
    step_sizes = jnp.clip(jnp.exp(jax.random.uniform(key_of[1], (ITERS,), jnp.float32, math.log(0.3), math.log(1.0))), 0.3, 1.0)
    facet_offsets = plant(jax.random.randint(key_of[2], (2, FACETS), 0, NIMG - FW + 1), jax.random.fold_in(key_of[2], 1), 0, NIMG - FW).astype(jnp.int32)
    col_offsets = plant(jax.random.randint(key_of[3], (NCOL,), 0, NIMG - SGW + 1), jax.random.fold_in(key_of[3], 1), 0, NIMG - SGW).astype(jnp.int32)
    row_offsets = plant(jax.random.randint(key_of[4], (NCOL, NROWSG), 0, NIMG - SGW + 1), jax.random.fold_in(key_of[4], 1), 0, NIMG - SGW).astype(jnp.int32)
    counts = draw_counts(jax.random.fold_in(key_of[9], 71), 0)
    vis_uv = plant(jax.random.randint(key_of[6], (2, NCOL, NROWSG, VCAP), OS * KSUP, OS * (SGW - KSUP)), jax.random.fold_in(key_of[6], 1), OS * KSUP, (OS * (SGW - KSUP)) - 1).astype(jnp.int32)
    vis_obs = bell_draw(key_of[7], (2, NCOL, NROWSG, VCAP), 1.0, 6.0, ((1, 4), (2, 8)))
    vis_weight = jnp.clip(jnp.exp(math.log(4.0) - 2.7725887 * jax.random.uniform(key_of[8], (NCOL, NROWSG, VCAP), jnp.float32) ** shard_levels(key_of[8], (NCOL, NROWSG, VCAP), ((0, 4), (1, 8)), -0.2, 0.2)), 0.25, 4.0).astype(jnp.bfloat16)
    return {"model_image": model_image, "step_sizes": step_sizes, "facet_offsets": facet_offsets, "col_offsets": col_offsets, "row_offsets": row_offsets, "counts": counts, "vis_uv": vis_uv, "vis_obs": vis_obs, "vis_weight": vis_weight}


two_pi = 2.0 * math.pi

def phase_index(frequency, pixels):
    pixel_low = pixels % 256
    pixel_high = pixels // 256
    return (frequency * pixel_low + frequency * pixel_high % (NIMG // 256) * 256) % NIMG

def row_table(frequency_start, pixel_start):
    frequency = frequency_start + jnp.arange(SGW, dtype=jnp.int32)
    pixels = pixel_start + jnp.arange(FROWS, dtype=jnp.int32)
    angles = phase_index(frequency[:, None], pixels[None, :]).astype(jnp.float32) * (two_pi / NIMG)
    return jnp.concatenate([jnp.cos(angles), jnp.sin(angles)], axis=1).astype(jnp.bfloat16)

def row_tables(frequency_starts, pixel_start):
    return jax.vmap(lambda single: row_table(single, pixel_start))(frequency_starts)

def column_table(frequency_start, pixel_start):
    frequency = frequency_start + jnp.arange(SGW, dtype=jnp.int32)
    pixels = pixel_start + jnp.arange(FW, dtype=jnp.int32)
    angles = phase_index(frequency[None, :], pixels[:, None]).astype(jnp.float32) * (two_pi / NIMG)
    return jnp.concatenate([jnp.cos(angles), -jnp.sin(angles)], axis=1).astype(jnp.bfloat16)

def expand_section(section_rows):
    real_half = section_rows[:, :SGW]
    imag_half = section_rows[:, SGW:]
    lower_rows = jnp.concatenate([imag_half, -real_half], axis=1)
    return jnp.concatenate([section_rows, lower_rows], axis=0)

def fold_back(back_rows):
    real_part = back_rows[..., :FROWS, :SGW] - back_rows[..., FROWS:, SGW:]
    imag_part = back_rows[..., :FROWS, SGW:] + back_rows[..., FROWS:, :SGW]
    return jnp.concatenate([real_part, imag_part], axis=-1)

def kernel_rows(position):
    offset = (jnp.arange(SGW, dtype=jnp.int32) * OS + OS // 2)[None, :] - position[:, None]
    distance = offset.astype(jnp.float32) / OS
    inside = jnp.abs(offset) <= KSUP * OS
    return jnp.where(inside, jnp.exp(-0.5 * distance * distance), 0.0).astype(jnp.bfloat16)

def block_pass(grid_bf, row_positions, column_positions, observed, weight, is_live):
    row_kernel = kernel_rows(row_positions)
    column_kernel = kernel_rows(column_positions)
    sampled = jnp.dot(row_kernel, grid_bf, preferred_element_type=jnp.float32)
    column_float = column_kernel.astype(jnp.float32)
    predicted_real = lax.optimization_barrier(jnp.sum(sampled[:, :SGW] * column_float, axis=1))
    predicted_imag = lax.optimization_barrier(jnp.sum(sampled[:, SGW:] * column_float, axis=1))
    weight_float = weight.astype(jnp.float32)
    residual_real = jnp.where(is_live, weight_float * (observed[0].astype(jnp.float32) - predicted_real), 0.0)
    residual_imag = jnp.where(is_live, weight_float * (observed[1].astype(jnp.float32) - predicted_imag), 0.0)
    weighted = jnp.concatenate([residual_real[:, None] * column_float, residual_imag[:, None] * column_float], axis=1).astype(jnp.bfloat16)
    block_grid = lax.dot_general(row_kernel, weighted, (((0,), (0,)), ((), ())), preferred_element_type=jnp.float32)
    return (block_grid, jnp.stack([residual_real, residual_imag]))

def sweep_blocks(grid_bf, positions, observed, weight, live_total, blocks):
    length = positions.shape[1]

    def one_block(block_index, running):
        grid_sum, residual = running
        first_row = (block_index * VB).astype(jnp.int32)
        position_part = lax.dynamic_slice_in_dim(positions, first_row, VB, 1)
        observed_part = lax.dynamic_slice_in_dim(observed, first_row, VB, 1)
        weight_part = lax.dynamic_slice_in_dim(weight, first_row, VB, 0)
        is_live = first_row + jnp.arange(VB, dtype=jnp.int32) < live_total
        block_grid, values = block_pass(grid_bf, position_part[0], position_part[1], observed_part, weight_part, is_live)
        residual = lax.dynamic_update_slice(residual, values, (jnp.int32(0), first_row))
        return (grid_sum + block_grid, residual)
    starting = (jnp.zeros((SGW, 2 * SGW), jnp.float32), jnp.zeros((2, length), jnp.float32))
    return lax.fori_loop(0, blocks, one_block, starting)

def reference(model_image, step_sizes, facet_offsets, col_offsets, row_offsets, counts, vis_uv, vis_obs, vis_weight):
    norm_factor = 1.0 / math.sqrt(FACETS * FROWS * FW)
    subgrid_total = NCOL * NROWSG
    facet_ids = jnp.arange(FACETS, dtype=jnp.int32)
    column_ids = jnp.arange(NCOL, dtype=jnp.int32)
    flat_positions = jnp.moveaxis(vis_uv.reshape(2, subgrid_total, VCAP), 1, 0)
    flat_observed = jnp.moveaxis(vis_obs.reshape(2, subgrid_total, VCAP), 1, 0)
    flat_weight = vis_weight.reshape(subgrid_total, VCAP)
    flat_counts = counts.reshape(subgrid_total)
    model_now = model_image
    residual = jnp.zeros((subgrid_total, 2, VCAP), jnp.float32)
    for cycle_index in range(ITERS):
        model_bf = model_now.astype(jnp.bfloat16)

        def facet_forward(running, facet_id):

            def column_forward(column_id):
                columns_factor = column_table(col_offsets[column_id], facet_offsets[1, facet_id])
                section_rows = jnp.dot(model_bf[facet_id], columns_factor, preferred_element_type=jnp.float32).astype(jnp.bfloat16)
                rows_factor = row_tables(row_offsets[column_id], facet_offsets[0, facet_id])
                product = jnp.dot(rows_factor.reshape(NROWSG * SGW, 2 * FROWS), expand_section(section_rows), preferred_element_type=jnp.float32)
                return product.reshape(NROWSG, SGW, 2 * SGW)
            return (running + lax.map(column_forward, column_ids), None)
        summed, unused = lax.scan(facet_forward, jnp.zeros((NCOL, NROWSG, SGW, 2 * SGW), jnp.float32), facet_ids)
        grids = (norm_factor * summed).astype(jnp.bfloat16).reshape(subgrid_total, SGW, 2 * SGW)

        def subgrid_pass(subgrid_items):
            grid_bf, positions, observed, weight, live_total = subgrid_items
            return sweep_blocks(grid_bf, positions, observed, weight, live_total, (live_total + VB - 1) // VB)
        gridded, residual = lax.map(subgrid_pass, (grids, flat_positions, flat_observed, flat_weight, flat_counts))
        gridded_bf = gridded.astype(jnp.bfloat16).reshape(NCOL, NROWSG, SGW, 2 * SGW)

        def facet_adjoint(facet_id):

            def column_adjoint(running, column_id):
                rows_factor = row_tables(row_offsets[column_id], facet_offsets[0, facet_id])
                back_rows = lax.dot_general(rows_factor.reshape(NROWSG * SGW, 2 * FROWS), gridded_bf[column_id].reshape(NROWSG * SGW, 2 * SGW), (((0,), (0,)), ((), ())), preferred_element_type=jnp.float32)
                adjoint_rows = fold_back(back_rows).astype(jnp.bfloat16)
                columns_factor = column_table(col_offsets[column_id], facet_offsets[1, facet_id])
                term = lax.dot_general(adjoint_rows, columns_factor, (((1,), (1,)), ((), ())), preferred_element_type=jnp.float32)
                return (running + term, None)
            total_rows, unused_rows = lax.scan(column_adjoint, jnp.zeros((FROWS, FW), jnp.float32), column_ids)
            return norm_factor * total_rows
        gradient = lax.map(facet_adjoint, facet_ids)
        model_now = model_now + step_sizes[cycle_index] * gradient
    residual_out = jnp.moveaxis(residual, 0, 1).reshape(2, NCOL, NROWSG, VCAP)
    return (model_now, residual_out)
```

```python
import functools
import math

import jax
import jax.numpy as jnp
from jax import lax
from jax.experimental import pallas as pl
from jax.experimental.pallas import tpu as pltpu
from jax.sharding import PartitionSpec as P

NIMG = 65536
SGW = 256
VB = 512
OS = 8
KSUP = 4
ITERS = 2
STEP = 1024
CHUNKS = 4
MESH = pl.DeviceIdType.MESH
VMEM = pltpu.VMEM
F32 = jnp.float32
BF16 = jnp.bfloat16
two_pi = 2.0 * math.pi


def cis(frequency, pixels):
    index = (frequency * pixels) & (NIMG - 1)
    angles = index.astype(F32) * (two_pi / NIMG)
    return jnp.concatenate([jnp.cos(angles), jnp.sin(angles)], axis=-1)


def dirichlet(k, start, length):
    k = ((k + NIMG // 2) & (NIMG - 1)) - NIMG // 2
    half = math.pi / NIMG
    phase = ((k * (2 * start + length - 1)) & (2 * NIMG - 1)).astype(F32) * half
    top = jnp.sin(((k * length) & (2 * NIMG - 1)).astype(F32) * half)
    bottom = jnp.sin(k.astype(F32) * half)
    zero = k == 0
    ratio = jnp.where(zero, float(length), top / jnp.where(zero, 1.0, bottom))
    phase = jnp.where(zero, 0.0, phase)
    return ratio * jnp.cos(phase), ratio * jnp.sin(phase)


def section_kernel(norm, model_ref, b_ref, c_ref, tw_ref, s_ref, st_ref, table):
    step = pl.program_id(0)
    fine = c_ref.shape[0]

    @pl.when(step == 0)
    def _():
        cc, cs = c_ref[:, :SGW], c_ref[:, SGW:]
        for h in range(STEP // fine):
            bc, bs = b_ref[h : h + 1, :SGW], b_ref[h : h + 1, SGW:]
            rows = pl.ds(h * fine, fine)
            table[rows, :SGW] = (bc * cc - bs * cs).astype(BF16)
            table[rows, SGW:] = (-(bc * cs + bs * cc)).astype(BF16)
        s_ref[...] = jnp.zeros_like(s_ref)

    part = jnp.dot(model_ref[...].astype(BF16), table[...], preferred_element_type=F32)
    pr, pi = part[:, :SGW], part[:, SGW:]
    tc, ts = tw_ref[0, :, :SGW], tw_ref[0, :, SGW:]
    s_ref[:, :SGW] += pr * tc + pi * ts
    s_ref[:, SGW:] += pi * tc - pr * ts

    @pl.when(step == pl.num_programs(0) - 1)
    def _():
        st_ref[...] = s_ref[...].T.astype(BF16)


def section(model, b, c, tw, norm):
    rows, width = model.shape
    return pl.pallas_call(
        functools.partial(section_kernel, norm),
        grid=(width // STEP,),
        out_shape=(
            jax.ShapeDtypeStruct((rows, 2 * SGW), F32),
            jax.ShapeDtypeStruct((2 * SGW, rows), BF16),
        ),
        in_specs=[
            pl.BlockSpec((rows, STEP), lambda i: (0, i)),
            pl.BlockSpec(b.shape, lambda i: (0, 0)),
            pl.BlockSpec(c.shape, lambda i: (0, 0)),
            pl.BlockSpec((1, 1, 2 * SGW), lambda i: (i, 0, 0)),
        ],
        out_specs=(
            pl.BlockSpec((rows, 2 * SGW), lambda i: (0, 0)),
            pl.BlockSpec((2 * SGW, rows), lambda i: (0, 0)),
        ),
        scratch_shapes=[VMEM((STEP, 2 * SGW), BF16)],
        name="section",
    )(model, b, c, tw)


def peers(n, ns):
    me = lax.axis_index("facet")
    z = lax.axis_index("sub")
    core = lax.rem(me, 2)
    chip = me // 2
    partner = me + 1 - 2 * core
    others = [lax.rem(chip + d, n // 2) * 2 + core for d in range(1, n // 2)]
    sources = [lax.rem(chip - d + n // 2, n // 2) * 2 + core for d in range(1, n // 2)]
    columns = [lax.rem(z + d, ns) for d in range(1, ns)]
    return me, z, core, chip, partner, others, sources, columns


def greet(partner, others, columns):
    barrier = pltpu.get_barrier_semaphore()
    for facet in [partner] + others:
        pl.semaphore_signal(barrier, inc=1, device_id={"facet": facet}, device_id_type=MESH)
    for column in columns:
        pl.semaphore_signal(barrier, inc=1, device_id={"sub": column}, device_id_type=MESH)
    pl.semaphore_wait(barrier, 1 + len(others) + len(columns))


def send(src, dst, send_sem, recv_sem, **where):
    return pltpu.make_async_remote_copy(
        src_ref=src,
        dst_ref=dst,
        send_sem=send_sem,
        recv_sem=recv_sem,
        device_id=where,
        device_id_type=MESH,
    )


def gather_kernel(n, ns, with_offsets, *refs):
    if with_offsets:
        x_ref, o_ref, out_ref, offs_ref, s1, r1, s2, r2, s3, r3 = refs
    else:
        x_ref, out_ref, s1, r1, s2, r2 = refs
    me, z, core, chip, partner, others, sources, columns = peers(n, ns)
    greet(partner, others, columns if with_offsets else [])
    first = []
    for d, other in enumerate(others):
        copy = send(x_ref, out_ref.at[me], s1.at[d + 1], r1.at[d + 1], facet=other)
        copy.start()
        first.append(copy)
    near = send(x_ref, out_ref.at[me], s1.at[0], r1.at[0], facet=partner)
    near.start()
    small = []
    if with_offsets:
        for d, column in enumerate(columns):
            copy = send(o_ref, offs_ref.at[z], s3.at[d], r3.at[d], sub=column)
            copy.start()
            small.append(copy)
        offs_ref[z] = o_ref[...]
    out_ref[me] = x_ref[...]
    second = []
    for d, source in enumerate(sources):
        send(x_ref, out_ref.at[source], s1.at[d + 1], r1.at[d + 1], facet=others[d]).wait_recv()
        copy = send(out_ref.at[source], out_ref.at[source], s2.at[d], r2.at[d], facet=partner)
        copy.start()
        second.append(copy)
    partner_core = 1 - core
    send(x_ref, out_ref.at[partner], s1.at[0], r1.at[0], facet=partner).wait_recv()
    for d, source in enumerate(sources):
        twin = source - core + partner_core
        send(out_ref.at[twin], out_ref.at[twin], s2.at[d], r2.at[d], facet=partner).wait_recv()
    if with_offsets:
        for d in range(ns - 1):
            source = lax.rem(z - d - 1 + ns, ns)
            send(o_ref, offs_ref.at[source], s3.at[d], r3.at[d], sub=columns[d]).wait_recv()
    for copy in first + [near] + second + small:
        copy.wait_send()


def gather(x, offsets, n, ns, collective_id):
    with_offsets = offsets is not None
    dma = pltpu.SemaphoreType.DMA
    operands = (x, offsets) if with_offsets else (x,)
    shapes = [jax.ShapeDtypeStruct((n,) + x.shape, x.dtype)]
    sems = [dma((n // 2,)), dma((n // 2,)), dma((n // 2,)), dma((n // 2,))]
    if with_offsets:
        shapes.append(jax.ShapeDtypeStruct((ns,) + offsets.shape, offsets.dtype))
        sems += [dma((ns,)), dma((ns,))]
    return pl.pallas_call(
        functools.partial(gather_kernel, n, ns, with_offsets),
        out_shape=tuple(shapes),
        in_specs=[pl.BlockSpec(memory_space=VMEM)] * len(operands),
        out_specs=tuple([pl.BlockSpec(memory_space=VMEM)] * len(shapes)),
        scratch_shapes=sems,
        compiler_params=pltpu.CompilerParams(collective_id=collective_id, has_side_effects=True),
        name="gather_sections",
    )(*operands)


def adjoint_kernel(n, ns, part_ref, out_ref, near_buf, send_buf, far_buf, ss1, rs1, ss2, rs2, sl, sr, rz):
    me, z, core, chip, partner, others, sources, columns = peers(n, ns)
    half = n // 2
    greet(partner, others, columns)
    partner_core = 1 - core
    order = list(range(1, half)) + [0]
    near = {}
    for d in order:
        dest = lax.rem(chip + d, half) * 2 + partner_core
        copy = send(part_ref.at[dest], near_buf.at[d], ss1.at[d], rs1.at[d], facet=partner)
        copy.start()
        near[d] = copy
    far = []
    for d in range(1, half):
        dest = lax.rem(chip + d, half) * 2 + core
        near[d].wait_recv()
        send_buf[d] = (part_ref[dest].astype(F32) + near_buf[d].astype(F32)).astype(BF16)
        copy = send(send_buf.at[d], far_buf.at[d], ss2.at[d], rs2.at[d], facet=dest)
        copy.start()
        far.append(copy)
    near[0].wait_recv()
    total = part_ref[me].astype(F32) + near_buf[0].astype(F32)
    for d in range(1, half):
        far[d - 1].wait_recv()
        total += far_buf[d].astype(F32)
    out_ref[z] = total.astype(BF16)
    rows = out_ref.shape[1] // CHUNKS

    def hop(source, k, right):
        piece = out_ref.at[source, pl.ds(k * rows, rows)]
        sem = sr if right else sl
        to = z + 1 if right else z - 1
        return send(piece, piece, sem.at[source, k], rz.at[source, k], sub=to)

    for k in range(CHUNKS):

        @pl.when(z < ns - 1)
        def _():
            hop(z, k, True).start()

        @pl.when(z > 0)
        def _():
            hop(z, k, False).start()

    for d in range(1, ns):
        for k in range(CHUNKS):

            @pl.when(z - d >= 0)
            def _():
                hop(z - d, k, True).wait_recv()

                @pl.when(z < ns - 1)
                def _():
                    hop(z - d, k, True).start()

            @pl.when(z + d < ns)
            def _():
                hop(z + d, k, False).wait_recv()

                @pl.when(z > 0)
                def _():
                    hop(z + d, k, False).start()

    for copy in list(near.values()) + far:
        copy.wait_send()
    for d in range(0, ns):
        for k in range(CHUNKS):

            @pl.when((z - d >= 0) & (z < ns - 1))
            def _():
                hop(z - d, k, True).wait_send()

            @pl.when((z + d < ns) & (z > 0))
            def _():
                hop(z + d, k, False).wait_send()


def adjoint(part, n, ns, collective_id):
    dma = pltpu.SemaphoreType.DMA
    half = n // 2
    block = part.shape[1:]
    return pl.pallas_call(
        functools.partial(adjoint_kernel, n, ns),
        out_shape=jax.ShapeDtypeStruct((ns,) + block, BF16),
        in_specs=[pl.BlockSpec(memory_space=VMEM)],
        out_specs=pl.BlockSpec(memory_space=VMEM),
        scratch_shapes=[
            VMEM((half,) + block, BF16),
            VMEM((half,) + block, BF16),
            VMEM((half,) + block, BF16),
            dma((half,)),
            dma((half,)),
            dma((half,)),
            dma((half,)),
            dma((ns, CHUNKS)),
            dma((ns, CHUNKS)),
            dma((ns, CHUNKS)),
        ],
        compiler_params=pltpu.CompilerParams(collective_id=collective_id, has_side_effects=True),
        name="adjoint_exchange",
    )(part)


def subgrid_kernel(
    norm, count_ref, y_ref, zb_ref, zc_ref, pos_ref, obs_ref, wt_ref, part_ref, res_ref, e_t, z_t, grid_t, acc
):
    n, _, rows = y_ref.shape
    fine = zc_ref.shape[0]
    cc, cs = zc_ref[:, :SGW], zc_ref[:, SGW:]
    for f in range(n):
        base = f * 2 * rows
        yr, yi = y_ref[f, :SGW, :], y_ref[f, SGW:, :]
        e_t[:SGW, base : base + rows] = yr
        e_t[:SGW, base + rows : base + 2 * rows] = yi
        e_t[SGW:, base : base + rows] = yi
        e_t[SGW:, base + rows : base + 2 * rows] = -yr
        for h in range(rows // fine):
            bc, bs = zb_ref[f, h : h + 1, :SGW], zb_ref[f, h : h + 1, SGW:]
            z_t[pl.ds(base + h * fine, fine), :] = (bc * cc - bs * cs).astype(BF16)
            z_t[pl.ds(base + rows + h * fine, fine), :] = (bc * cs + bs * cc).astype(BF16)
    grid_t[...] = (norm * jnp.dot(e_t[...], z_t[...], preferred_element_type=F32)).astype(BF16)
    acc[...] = jnp.zeros_like(acc)
    cells = lax.broadcasted_iota(jnp.int32, (SGW, VB), 0).astype(F32) + 0.5
    lanes = lax.broadcasted_iota(jnp.int32, (1, VB), 1)
    count = count_ref[0, 0]

    def kernel_of(position):
        distance = cells - position.astype(F32) * (1.0 / OS)
        square = distance * distance
        return jnp.where(square <= float(KSUP * KSUP), jnp.exp(-0.5 * square), 0.0).astype(BF16)

    def block(i, carry):
        start = pl.multiple_of(i * VB, VB)
        part = pl.ds(start, VB)
        ku = kernel_of(pos_ref[0:1, part])
        kv = kernel_of(pos_ref[1:2, part]).astype(F32)
        h = jnp.dot(grid_t[...], ku, preferred_element_type=F32)
        pr = jnp.sum(h[:SGW] * kv, axis=0, keepdims=True)
        pi = jnp.sum(h[SGW:] * kv, axis=0, keepdims=True)
        live = lanes + start < count
        weight = wt_ref[0:1, part].astype(F32)
        rr = jnp.where(live, weight * (obs_ref[0:1, part].astype(F32) - pr), 0.0)
        ri = jnp.where(live, weight * (obs_ref[1:2, part].astype(F32) - pi), 0.0)
        res_ref[0:1, part] = rr
        res_ref[1:2, part] = ri
        weighted = jnp.concatenate([(rr * kv).astype(BF16), (ri * kv).astype(BF16)], axis=0)
        acc[...] += lax.dot_general(ku, weighted, (((1,), (1,)), ((), ())), preferred_element_type=F32)
        return carry

    lax.fori_loop(0, pos_ref.shape[1] // VB, block, 0)
    gridded = acc[...].astype(BF16)
    for f in range(n):
        back = jnp.dot(z_t[pl.ds(f * 2 * rows, 2 * rows), :], gridded, preferred_element_type=F32)
        part_ref[f, :, :SGW] = (back[:rows, :SGW] - back[rows:, SGW:]).astype(BF16)
        part_ref[f, :, SGW:] = (back[:rows, SGW:] + back[rows:, :SGW]).astype(BF16)


def subgrid(count, y, zb, zc, positions, observed, weight, norm):
    n, _, rows = y.shape
    slots = positions.shape[1]
    vmem = pl.BlockSpec(memory_space=VMEM)
    return pl.pallas_call(
        functools.partial(subgrid_kernel, norm),
        out_shape=(
            jax.ShapeDtypeStruct((n, rows, 2 * SGW), BF16),
            jax.ShapeDtypeStruct((2, slots), F32),
        ),
        in_specs=[pl.BlockSpec(memory_space=pltpu.SMEM)] + [vmem] * 6,
        out_specs=(vmem, vmem),
        scratch_shapes=[
            VMEM((2 * SGW, n * 2 * rows), BF16),
            VMEM((n * 2 * rows, SGW), BF16),
            VMEM((2 * SGW, SGW), BF16),
            VMEM((SGW, 2 * SGW), F32),
        ],
        name="subgrid",
    )(count, y, zb, zc, positions, observed, weight)


def update_kernel(norm, step_ref, s_ref, a_ref, d_ref, st_ref):
    ns = a_ref.shape[0]
    rev = (
        lax.broadcasted_iota(jnp.int32, (SGW, SGW), 0) + lax.broadcasted_iota(jnp.int32, (SGW, SGW), 1) == SGW - 1
    ).astype(F32).astype(BF16)

    def toeplitz(c, i):
        wide = jnp.broadcast_to(d_ref[c, i : i + 1, :], (SGW, 2 * SGW))
        return pltpu.roll(wide, 0, 1, stride=1, stride_axis=0)[:, :SGW]

    def mm(a, b):
        return jnp.dot(a, b, preferred_element_type=F32)

    sr = jnp.zeros((s_ref.shape[0], SGW), F32)
    si = jnp.zeros((s_ref.shape[0], SGW), F32)
    for c in range(ns):
        ar, ai = a_ref[c, :, :SGW], a_ref[c, :, SGW:]
        vr, vi = mm(ar, rev).astype(BF16), mm(ai, rev).astype(BF16)
        d1r, d1i = toeplitz(c, 0).astype(BF16), toeplitz(c, 1).astype(BF16)
        d2r, d2i = toeplitz(c, 2).astype(BF16), toeplitz(c, 3).astype(BF16)
        sr += mm(ar, d1r) - mm(ai, d1i) + mm(vr, d2r) + mm(vi, d2i)
        si += mm(ar, d1i) + mm(ai, d1r) + mm(vr, d2i) - mm(vi, d2r)
    scale = step_ref[0, 0] * (0.5 * norm)
    st_ref[:SGW, :] = (s_ref[:, :SGW] + scale * sr).T.astype(BF16)
    st_ref[SGW:, :] = (s_ref[:, SGW:] + scale * si).T.astype(BF16)


def update(step, s, a, d, norm):
    vmem = pl.BlockSpec(memory_space=VMEM)
    return pl.pallas_call(
        functools.partial(update_kernel, norm),
        out_shape=jax.ShapeDtypeStruct((2 * SGW, s.shape[0]), BF16),
        in_specs=[pl.BlockSpec(memory_space=pltpu.SMEM)] + [vmem] * 3,
        out_specs=vmem,
        name="next_section",
    )(step, s, a, d)


def image_kernel(norm, steps_ref, model_ref, a0_ref, a1_ref, tw_ref, bt_ref, ct_ref, out_ref, turned, table):
    ns, rows, _ = a0_ref.shape
    blocks = model_ref.shape[1] // STEP
    s0, s1 = steps_ref[0, 0] * norm, steps_ref[0, 1] * norm
    fine = ct_ref.shape[2]
    for c in range(ns):
        a = s0 * a0_ref[c].astype(F32) + s1 * a1_ref[c].astype(F32)
        ar, ai = a[:, :SGW], a[:, SGW:]
        base = c * 2 * SGW
        for j in range(blocks):
            tc, ts = tw_ref[c, j : j + 1, :SGW], tw_ref[c, j : j + 1, SGW:]
            part = pl.ds(j * rows, rows)
            turned[part, base : base + SGW] = (ar * tc - ai * ts).astype(BF16)
            turned[part, base + SGW : base + 2 * SGW] = (ar * ts + ai * tc).astype(BF16)
        cc, cs = ct_ref[c, :SGW, :], ct_ref[c, SGW:, :]
        for h in range(STEP // fine):
            bc = bt_ref[c, :SGW, h : h + 1]
            bs = bt_ref[c, SGW:, h : h + 1]
            part = slice(h * fine, (h + 1) * fine)
            table[base : base + SGW, part] = (bc * cc - bs * cs).astype(BF16)
            table[base + SGW : base + 2 * SGW, part] = (-(bc * cs + bs * cc)).astype(BF16)
    width = 256

    def chunk(i, carry):
        first = pl.multiple_of(i * width, width)
        got = jnp.dot(turned[...], table[:, pl.ds(first, width)], preferred_element_type=F32)
        for j in range(blocks):
            where = pl.ds(pl.multiple_of(j * STEP + i * width, width), width)
            out_ref[:, where] = model_ref[:, where] + got[j * rows : (j + 1) * rows]
        return carry

    lax.fori_loop(0, STEP // width, chunk, 0)


def image(steps, model, a0, a1, tw, bt, ct, norm):
    ns, rows, _ = a0.shape
    vmem = pl.BlockSpec(memory_space=VMEM)
    blocks = model.shape[1] // STEP
    return pl.pallas_call(
        functools.partial(image_kernel, norm),
        out_shape=jax.ShapeDtypeStruct(model.shape, F32),
        in_specs=[pl.BlockSpec(memory_space=pltpu.SMEM)] + [vmem] * 6,
        out_specs=vmem,
        scratch_shapes=[
            VMEM((blocks * rows, ns * 2 * SGW), BF16),
            VMEM((ns * 2 * SGW, STEP), BF16),
        ],
        name="image",
    )(steps, model, a0, a1, tw, bt, ct)


def local(model_image, step_sizes, facet_offsets, col_offsets, row_offsets, counts, vis_uv, vis_obs, vis_weight):
    n = lax.axis_size("facet")
    ns = lax.axis_size("sub")
    model = model_image[0]
    rows, width = model.shape
    norm = 1.0 / math.sqrt(n * rows * width)
    me = lax.axis_index("facet")
    cells = jnp.arange(SGW, dtype=jnp.int32)
    fine = 32
    blocks = width // STEP
    pixel = facet_offsets[1, me]
    own = col_offsets[0] + cells
    coarse_pixels = pixel + fine * jnp.arange(STEP // fine, dtype=jnp.int32)
    b = cis(own[None, :], coarse_pixels[:, None])
    c = cis(own[None, :], jnp.arange(fine, dtype=jnp.int32)[:, None])
    block_starts = STEP * jnp.arange(blocks, dtype=jnp.int32)
    tw = cis(own[None, :], block_starts[:, None])[:, None, :]
    row_fine = 16
    row_q = row_offsets[0, me] + cells
    row_pixels = facet_offsets[0][:, None] + row_fine * jnp.arange(rows // row_fine, dtype=jnp.int32)[None, :]
    zb = cis(row_q[None, None, :], row_pixels[:, :, None])
    zc = cis(row_q[None, :], jnp.arange(row_fine, dtype=jnp.int32)[:, None])

    positions = vis_uv[:, 0, 0]
    observed = vis_obs[:, 0, 0]
    weight = vis_weight[0]
    count = lax.dynamic_slice(counts, (jnp.int32(0), me), (1, 1))
    steps = step_sizes[None, :]

    s0, st0 = section(model, b, c, tw, norm)
    offsets = jnp.broadcast_to(col_offsets[:, None], (8, 128))
    gathered, columns = gather(st0, offsets, n, ns, 0)
    columns = columns[:, 0, 0]
    part, _ = subgrid(count, gathered, zb, zc, positions, observed, weight, norm)

    lags = jnp.arange(2 * SGW, dtype=jnp.int32)
    lags = jnp.where(lags < SGW, lags, lags - 2 * SGW)[None, :]
    d1 = dirichlet((columns - col_offsets[0])[:, None] - lags, pixel, width)
    d2 = dirichlet(-((columns + col_offsets[0])[:, None] + SGW - 1 + lags), pixel, width)
    d = jnp.stack([d1[0], d1[1], d2[0], d2[1]], axis=1)

    a0 = adjoint(part, n, ns, 1)
    st1 = update(steps, s0, a0, d, norm)
    (gathered,) = gather(st1, None, n, ns, 2)
    part, residual = subgrid(count, gathered, zb, zc, positions, observed, weight, norm)
    a1 = adjoint(part, n, ns, 1)

    every = columns[:, None] + cells[None, :]
    lane_fine = 128
    twa = cis(every[:, None, :], block_starts[None, :, None])
    bt_pixels = pixel + lane_fine * jnp.arange(STEP // lane_fine, dtype=jnp.int32)
    every = every[:, :, None]

    def stacked(pixels):
        angles = ((every * pixels) & (NIMG - 1)).astype(F32) * (two_pi / NIMG)
        return jnp.concatenate([jnp.cos(angles), jnp.sin(angles)], axis=1)

    bt = stacked(bt_pixels[None, None, :])
    ct = stacked(jnp.arange(lane_fine, dtype=jnp.int32)[None, None, :])
    out = image(steps, model, a0, a1, twa, bt, ct, norm)
    return (out[None], residual.reshape(2, 1, 1, residual.shape[1]))


def solution(mesh):
    in_specs = (
        P("facet", None, None),
        P(),
        P(),
        P("sub"),
        P("sub", None),
        P("sub", None),
        P(None, "sub", "facet", None),
        P(None, "sub", "facet", None),
        P("sub", "facet", None),
    )
    out_specs = (P("facet", None, None), P(None, "sub", "facet", None))
    return jax.shard_map(local, mesh=mesh, in_specs=in_specs, out_specs=out_specs, check_vma=False)
```

```python
import functools
import math

import jax
import jax.numpy as jnp
from jax import lax
from jax.experimental import pallas as pl
from jax.experimental.pallas import tpu as pltpu
from jax.sharding import PartitionSpec as P

NIMG = 65536
SGW = 256
VB = 512
OS = 8
KSUP = 4
ITERS = 2
STEP = 1024
CHUNKS = 4
MESH = pl.DeviceIdType.MESH
VMEM = pltpu.VMEM
F32 = jnp.float32
BF16 = jnp.bfloat16
two_pi = 2.0 * math.pi


def iota(shape, dim):
    return lax.broadcasted_iota(jnp.int32, shape, dim)


def cis(frequency, pixels):
    index = (frequency * pixels) & (NIMG - 1)
    angles = index.astype(F32) * (two_pi / NIMG)
    return jnp.cos(angles), jnp.sin(angles)


def dirichlet(k, start, length):
    k = ((k + NIMG // 2) & (NIMG - 1)) - NIMG // 2
    half = math.pi / NIMG
    phase = ((k * (2 * start + length - 1)) & (2 * NIMG - 1)).astype(F32) * half
    top = jnp.sin(((k * length) & (2 * NIMG - 1)).astype(F32) * half)
    bottom = jnp.sin(k.astype(F32) * half)
    zero = k == 0
    ratio = jnp.where(zero, float(length), top / jnp.where(zero, 1.0, bottom))
    phase = jnp.where(zero, 0.0, phase)
    return ratio * jnp.cos(phase), ratio * jnp.sin(phase)


def mm(a, b):
    return jnp.dot(a, b, preferred_element_type=F32)


def peers(n, ns):
    me = lax.axis_index("facet")
    z = lax.axis_index("sub")
    core = lax.rem(me, 2)
    chip = me // 2
    partner = me + 1 - 2 * core
    others = [lax.rem(chip + d, n // 2) * 2 + core for d in range(1, n // 2)]
    sources = [lax.rem(chip - d + n // 2, n // 2) * 2 + core for d in range(1, n // 2)]
    columns = [lax.rem(z + d, ns) for d in range(1, ns)]
    return me, z, core, chip, partner, others, sources, columns


def greet(partner, others, columns):
    barrier = pltpu.get_barrier_semaphore()
    for facet in [partner] + others:
        pl.semaphore_signal(barrier, inc=1, device_id={"facet": facet}, device_id_type=MESH)
    for column in columns:
        pl.semaphore_signal(barrier, inc=1, device_id={"sub": column}, device_id_type=MESH)
    pl.semaphore_wait(barrier, 1 + len(others) + len(columns))


def send(src, dst, send_sem, recv_sem, **where):
    return pltpu.make_async_remote_copy(
        src_ref=src,
        dst_ref=dst,
        send_sem=send_sem,
        recv_sem=recv_sem,
        device_id=where,
        device_id_type=MESH,
    )


def step_kernel(
    n, ns, steps_ref, facet_ref, col_ref, row_ref, count_ref, model_ref, pos_ref, obs_ref, wt_ref,
    out_ref, res_ref,
    mb, table, s_ref, st, got_y, o_ref, offs, z_t, gacc, grid_t, ku_t, kv_t, acc, part_p, part_o,
    near_buf, send_buf, far_buf, adj, lag_t, tw_t, image_t, turned,
    ms, s1, r1, s2, r2, s3, r3, ss1, rs1, ss2, rs2, sl, sr, rz,
):
    rows, width = out_ref.shape
    blocks = width // STEP
    slots = pos_ref.shape[-1]
    half = n // 2
    norm = 1.0 / math.sqrt(n * rows * width)
    me, z, core, chip, partner, others, sources, columns = peers(n, ns)
    partner_core = 1 - core
    pixel = facet_ref[1, me]
    own = col_ref[0]

    loads = []
    for j in range(blocks):
        where = pl.ds(j * STEP, STEP)
        load = pltpu.make_async_copy(model_ref.at[:, where], out_ref.at[:, where], ms.at[j])
        load.start()
        loads.append(load)
    o_ref[...] = jnp.full(o_ref.shape, own, jnp.int32)

    fine = 32
    q = iota((fine, SGW), 1) + own
    bc, bs = cis(q, pixel + fine * iota((STEP // fine, SGW), 0))
    cc, cs = cis(q, iota((fine, SGW), 0))
    for h in range(STEP // fine):
        hc, hs = bc[h : h + 1], bs[h : h + 1]
        table[h * fine : (h + 1) * fine, :SGW] = (hc * cc - hs * cs).astype(BF16)
        table[h * fine : (h + 1) * fine, SGW:] = (-(hc * cs + hs * cc)).astype(BF16)
    tc, ts = cis(iota((blocks, SGW), 1) + own, STEP * iota((blocks, SGW), 0))
    for j in range(blocks):
        loads[j].wait()
        mb[j * rows : (j + 1) * rows, :] = out_ref[:, j * STEP : (j + 1) * STEP].astype(BF16)
    yr = jnp.zeros((rows, SGW), F32)
    yi = jnp.zeros((rows, SGW), F32)
    group = max(blocks // 2, 1)
    for first in range(0, blocks, group):
        part = mm(mb[first * rows : (first + group) * rows, :], table[...])
        for j in range(group):
            pr, pi = part[j * rows : (j + 1) * rows, :SGW], part[j * rows : (j + 1) * rows, SGW:]
            c, s = tc[first + j : first + j + 1], ts[first + j : first + j + 1]
            yr += pr * c + pi * s
            yi += pi * c - pr * s
    s_ref[:, :SGW] = yr
    s_ref[:, SGW:] = yi
    st[0, :SGW, :] = yr.T.astype(BF16)
    st[0, SGW:, :] = yi.T.astype(BF16)
    greet(partner, others, columns)

    def subgrid_tables():
        row_fine = 16
        q = iota((row_fine, SGW), 1) + row_ref[0, me]
        cc, cs = cis(q, iota((row_fine, SGW), 0))
        for f in range(n):
            steps = rows // row_fine
            bc, bs = cis(
                iota((steps, SGW), 1) + row_ref[0, me], facet_ref[0, f] + row_fine * iota((steps, SGW), 0)
            )
            for h in range(steps):
                hc, hs = bc[h : h + 1], bs[h : h + 1]
                at = h * row_fine
                z_t[f, at : at + row_fine, :] = (hc * cc - hs * cs).astype(BF16)
                z_t[f, rows + at : rows + at + row_fine, :] = (hc * cs + hs * cc).astype(BF16)
        cells = iota((SGW, VB), 0).astype(F32) + 0.5

        def kernel_of(position):
            distance = cells - position.astype(F32) * (1.0 / OS)
            square = distance * distance
            return jnp.where(square <= float(KSUP * KSUP), jnp.exp(-0.5 * square), 0.0).astype(BF16)

        def block(i, carry):
            part = pl.ds(pl.multiple_of(i * VB, VB), VB)
            ku_t[:, part] = kernel_of(pos_ref[0, 0, 0:1, part])
            kv_t[:, part] = kernel_of(pos_ref[1, 0, 0:1, part])
            return carry

        lax.fori_loop(0, slots // VB, block, 0)

    def lag_tables():
        lags = iota((1, 2 * SGW), 1)
        lags = jnp.where(lags < SGW, lags, lags - 2 * SGW)

        def column(c, carry):
            other = jnp.broadcast_to(offs[c][0:1, 0:1], (1, 2 * SGW))
            d1 = dirichlet(other - own - lags, pixel, width)
            d2 = dirichlet(-(other + own + SGW - 1 + lags), pixel, width)
            for i, line in enumerate(d1 + d2):
                wide = jnp.broadcast_to(line, (SGW, 2 * SGW))
                lag_t[c, i] = pltpu.roll(wide, 0, 1, stride=1, stride_axis=0)[:, :SGW].astype(BF16)
            return carry

        lax.fori_loop(0, ns, column, 0)

    def image_tables():
        lane_fine = 128
        coarse = STEP // lane_fine

        def column(c, carry):
            other = offs[c][0:1, 0:1]
            tc, ts = cis(iota((blocks, SGW), 1) + other, STEP * iota((blocks, SGW), 0))
            tw_t[c, :, :SGW] = tc
            tw_t[c, :, SGW:] = ts
            q = iota((SGW, lane_fine), 0) + other
            bc, bs = cis(q, pixel + lane_fine * iota((SGW, lane_fine), 1))
            cc, cs = cis(q, iota((SGW, lane_fine), 1))
            for h in range(coarse):
                hc, hs = bc[:, h : h + 1], bs[:, h : h + 1]
                part = slice(h * lane_fine, (h + 1) * lane_fine)
                image_t[c, :SGW, part] = (hc * cc - hs * cs).astype(BF16)
                image_t[c, SGW:, part] = (-(hc * cs + hs * cc)).astype(BF16)
            return carry

        lax.fori_loop(0, ns, column, 0)

    def grid_term(t, f):
        yr, yi = got_y[t, f, :SGW, :], got_y[t, f, SGW:, :]
        zf = z_t[f]
        gacc[:SGW] += mm(jnp.concatenate([yr, yi], axis=1), zf)
        gacc[SGW:] += mm(jnp.concatenate([yi, -yr], axis=1), zf)

    def gather_sections(t, meanwhile):
        sent = []
        for d, other in enumerate(others):
            copy = send(st.at[t], got_y.at[t, me], s1.at[t, d + 1], r1.at[t, d + 1], facet=other)
            copy.start()
            sent.append(copy)
        near = send(st.at[t], got_y.at[t, me], s1.at[t, 0], r1.at[t, 0], facet=partner)
        near.start()
        sent.append(near)
        small = []
        if t == 0:
            for d, column in enumerate(columns):
                copy = send(o_ref, offs.at[z], s3.at[d], r3.at[d], sub=column)
                copy.start()
                sent.append(copy)
            offs[z] = o_ref[...]
        got_y[t, me] = st[t]
        meanwhile()
        gacc[...] = jnp.zeros_like(gacc)
        grid_term(t, me)
        send(st.at[t], got_y.at[t, partner], s1.at[t, 0], r1.at[t, 0], facet=partner).wait_recv()
        grid_term(t, partner)
        for d, source in enumerate(sources):
            send(st.at[t], got_y.at[t, source], s1.at[t, d + 1], r1.at[t, d + 1], facet=others[d]).wait_recv()
            block = got_y.at[t, source]
            copy = send(block, block, s2.at[t, d], r2.at[t, d], facet=partner)
            copy.start()
            sent.append(copy)
            grid_term(t, source)
        for d, source in enumerate(sources):
            twin = source - core + partner_core
            block = got_y.at[t, twin]
            send(block, block, s2.at[t, d], r2.at[t, d], facet=partner).wait_recv()
            grid_term(t, twin)
        if t == 0:
            for d in range(ns - 1):
                source = lax.rem(z - d - 1 + ns, ns)
                send(o_ref, offs.at[source], s3.at[d], r3.at[d], sub=columns[d]).wait_recv()
        for copy in sent:
            copy.wait_send()
        grid_t[...] = (norm * gacc[...]).astype(BF16)

    def sweep(last):
        acc[...] = jnp.zeros_like(acc)
        lanes = iota((1, VB), 1)
        count = count_ref[0, me]

        def block(i, carry):
            start = pl.multiple_of(i * VB, VB)
            part = pl.ds(start, VB)
            ku = ku_t[:, part]
            kv = kv_t[:, part].astype(F32)
            h = mm(grid_t[...], ku)
            pr = jnp.sum(h[:SGW] * kv, axis=0, keepdims=True)
            pi = jnp.sum(h[SGW:] * kv, axis=0, keepdims=True)
            live = lanes + start < count
            weight = wt_ref[0, 0:1, part].astype(F32)
            rr = jnp.where(live, weight * (obs_ref[0, 0, 0:1, part].astype(F32) - pr), 0.0)
            ri = jnp.where(live, weight * (obs_ref[1, 0, 0:1, part].astype(F32) - pi), 0.0)
            if last:
                res_ref[0, 0, 0:1, part] = rr
                res_ref[1, 0, 0:1, part] = ri
            weighted = jnp.concatenate([(rr * kv).astype(BF16), (ri * kv).astype(BF16)], axis=0)
            acc[...] += lax.dot_general(ku, weighted, (((1,), (1,)), ((), ())), preferred_element_type=F32)
            return carry

        lax.fori_loop(0, slots // VB, block, 0)

    def exchange(t, meanwhile, use_column):
        gridded = acc[...].astype(BF16)

        def fold(dest):
            back = mm(z_t[dest], gridded)
            return back[:rows, :SGW] - back[rows:, SGW:], back[:rows, SGW:] + back[rows:, :SGW]

        order = list(range(1, half)) + [0]
        near = {}
        for d in order:
            real, imag = fold(lax.rem(chip + d, half) * 2 + partner_core)
            part_p[t, d, :, :SGW] = real.astype(BF16)
            part_p[t, d, :, SGW:] = imag.astype(BF16)
            near[d] = send(part_p.at[t, d], near_buf.at[t, d], ss1.at[t, d], rs1.at[t, d], facet=partner)
            near[d].start()
        for d in order:
            real, imag = fold(lax.rem(chip + d, half) * 2 + core)
            part_o[d, :, :SGW] = real
            part_o[d, :, SGW:] = imag
        far = []
        for d in range(1, half):
            dest = lax.rem(chip + d, half) * 2 + core
            near[d].wait_recv()
            send_buf[t, d] = (part_o[d] + near_buf[t, d].astype(F32)).astype(BF16)
            copy = send(send_buf.at[t, d], far_buf.at[t, d], ss2.at[t, d], rs2.at[t, d], facet=dest)
            copy.start()
            far.append(copy)
        meanwhile()
        near[0].wait_recv()
        total = part_o[0] + near_buf[t, 0].astype(F32)
        for d in range(1, half):
            far[d - 1].wait_recv()
            total += far_buf[t, d].astype(F32)
        adj[t, z] = total.astype(BF16)
        size = rows // CHUNKS

        def hop(source, k, right):
            piece = adj.at[t, source, pl.ds(k * size, size)]
            sem = sr if right else sl
            to = z + 1 if right else z - 1
            return send(piece, piece, sem.at[t, source, k], rz.at[t, source, k], sub=to)

        for k in range(CHUNKS):

            @pl.when(z < ns - 1)
            def _():
                hop(z, k, True).start()

            @pl.when(z > 0)
            def _():
                hop(z, k, False).start()

        use_column(z)
        for d in range(1, ns):
            for k in range(CHUNKS):

                @pl.when(z - d >= 0)
                def _():
                    hop(z - d, k, True).wait_recv()

                    @pl.when(z < ns - 1)
                    def _():
                        hop(z - d, k, True).start()

                @pl.when(z + d < ns)
                def _():
                    hop(z + d, k, False).wait_recv()

                    @pl.when(z > 0)
                    def _():
                        hop(z + d, k, False).start()

            @pl.when(z - d >= 0)
            def _():
                use_column(z - d)

            @pl.when(z + d < ns)
            def _():
                use_column(z + d)

        for copy in list(near.values()) + far:
            copy.wait_send()
        for d in range(0, ns):
            for k in range(CHUNKS):

                @pl.when((z - d >= 0) & (z < ns - 1))
                def _():
                    hop(z - d, k, True).wait_send()

                @pl.when((z + d < ns) & (z > 0))
                def _():
                    hop(z + d, k, False).wait_send()

    mirror = (iota((SGW, SGW), 0) + iota((SGW, SGW), 1) == SGW - 1).astype(F32).astype(BF16)

    def add_to_section(c):
        scale = steps_ref[0] * (0.5 * norm)
        ar, ai = adj[0, c, :, :SGW], adj[0, c, :, SGW:]
        vr, vi = mm(ar, mirror).astype(BF16), mm(ai, mirror).astype(BF16)
        d1r, d1i, d2r, d2i = lag_t[c, 0], lag_t[c, 1], lag_t[c, 2], lag_t[c, 3]
        s_ref[:, :SGW] += scale * (mm(ar, d1r) - mm(ai, d1i) + mm(vr, d2r) + mm(vi, d2i))
        s_ref[:, SGW:] += scale * (mm(ar, d1i) + mm(ai, d1r) + mm(vr, d2i) - mm(vi, d2r))

    def add_to_image(c):
        a = (steps_ref[0] * norm) * adj[0, c].astype(F32) + (steps_ref[1] * norm) * adj[1, c].astype(F32)
        ar, ai = a[:, :SGW], a[:, SGW:]
        for j in range(blocks):
            tc, ts = tw_t[c, j : j + 1, :SGW], tw_t[c, j : j + 1, SGW:]
            turned[j * rows : (j + 1) * rows, :SGW] = (ar * tc - ai * ts).astype(BF16)
            turned[j * rows : (j + 1) * rows, SGW:] = (ar * ts + ai * tc).astype(BF16)
        lanes = 256

        def chunk(i, carry):
            got = mm(turned[...], image_t[c, :, pl.ds(pl.multiple_of(i * lanes, lanes), lanes)])
            for j in range(blocks):
                where = pl.ds(pl.multiple_of(j * STEP + i * lanes, lanes), lanes)
                out_ref[:, where] += got[j * rows : (j + 1) * rows]
            return carry

        lax.fori_loop(0, STEP // lanes, chunk, 0)

    gather_sections(0, subgrid_tables)
    sweep(False)
    exchange(0, lag_tables, add_to_section)
    st[1, :SGW, :] = s_ref[:, :SGW].T.astype(BF16)
    st[1, SGW:, :] = s_ref[:, SGW:].T.astype(BF16)
    gather_sections(1, image_tables)
    sweep(True)
    exchange(1, lambda: None, add_to_image)


def local(model_image, step_sizes, facet_offsets, col_offsets, row_offsets, counts, vis_uv, vis_obs, vis_weight):
    n = lax.axis_size("facet")
    ns = lax.axis_size("sub")
    model = model_image[0]
    rows, width = model.shape
    slots = vis_uv.shape[-1]
    half = n // 2
    blocks = width // STEP
    dma = pltpu.SemaphoreType.DMA
    vmem = pl.BlockSpec(memory_space=VMEM)
    smem = pl.BlockSpec(memory_space=pltpu.SMEM)
    image, residual = pl.pallas_call(
        functools.partial(step_kernel, n, ns),
        out_shape=(
            jax.ShapeDtypeStruct(model.shape, F32),
            jax.ShapeDtypeStruct((2, 1, 1, slots), F32),
        ),
        in_specs=[smem] * 5 + [pl.BlockSpec(memory_space=pl.ANY)] + [vmem] * 3,
        out_specs=(vmem, vmem),
        scratch_shapes=[
            VMEM((blocks * rows, STEP), BF16),
            VMEM((STEP, 2 * SGW), BF16),
            VMEM((rows, 2 * SGW), F32),
            VMEM((ITERS, 2 * SGW, rows), BF16),
            VMEM((ITERS, n, 2 * SGW, rows), BF16),
            VMEM((8, 128), jnp.int32),
            VMEM((ns, 8, 128), jnp.int32),
            VMEM((n, 2 * rows, SGW), BF16),
            VMEM((2 * SGW, SGW), F32),
            VMEM((2 * SGW, SGW), BF16),
            VMEM((SGW, slots), BF16),
            VMEM((SGW, slots), BF16),
            VMEM((SGW, 2 * SGW), F32),
            VMEM((ITERS, half, rows, 2 * SGW), BF16),
            VMEM((half, rows, 2 * SGW), F32),
            VMEM((ITERS, half, rows, 2 * SGW), BF16),
            VMEM((ITERS, half, rows, 2 * SGW), BF16),
            VMEM((ITERS, half, rows, 2 * SGW), BF16),
            VMEM((ITERS, ns, rows, 2 * SGW), BF16),
            VMEM((ns, 4, SGW, SGW), BF16),
            VMEM((ns, blocks, 2 * SGW), F32),
            VMEM((ns, 2 * SGW, STEP), BF16),
            VMEM((blocks * rows, 2 * SGW), BF16),
            dma((blocks,)),
            dma((ITERS, half)),
            dma((ITERS, half)),
            dma((ITERS, half)),
            dma((ITERS, half)),
            dma((ns,)),
            dma((ns,)),
            dma((ITERS, half)),
            dma((ITERS, half)),
            dma((ITERS, half)),
            dma((ITERS, half)),
            dma((ITERS, ns, CHUNKS)),
            dma((ITERS, ns, CHUNKS)),
            dma((ITERS, ns, CHUNKS)),
        ],
        compiler_params=pltpu.CompilerParams(collective_id=0, has_side_effects=True),
        name="cycles",
    )(step_sizes, facet_offsets, col_offsets, row_offsets, counts, model, vis_uv, vis_obs, vis_weight)
    return (image[None], residual)


def solution(mesh):
    in_specs = (
        P("facet", None, None),
        P(),
        P(),
        P("sub"),
        P("sub", None),
        P("sub", None),
        P(None, "sub", "facet", None),
        P(None, "sub", "facet", None),
        P("sub", "facet", None),
    )
    out_specs = (P("facet", None, None), P(None, "sub", "facet", None))
    return jax.shard_map(local, mesh=mesh, in_specs=in_specs, out_specs=out_specs, check_vma=False)
```

```python
import functools
import math

import jax
import jax.numpy as jnp
from jax import lax
from jax.experimental import pallas as pl
from jax.experimental.pallas import tpu as pltpu
from jax.sharding import PartitionSpec as P

NIMG = 65536
SGW = 256
VB = 512
OS = 8
KSUP = 4
ITERS = 2
STEP = 1024
CHUNKS = 4
VMEM_BYTES = 67043328
MESH = pl.DeviceIdType.MESH
VMEM = pltpu.VMEM
F32 = jnp.float32
BF16 = jnp.bfloat16
two_pi = 2.0 * math.pi


def iota(shape, dim):
    return lax.broadcasted_iota(jnp.int32, shape, dim)


def cis(frequency, pixels):
    index = (frequency * pixels) & (NIMG - 1)
    angles = index.astype(F32) * (two_pi / NIMG)
    return jnp.cos(angles), jnp.sin(angles)


def dirichlet(k, start, length):
    k = ((k + NIMG // 2) & (NIMG - 1)) - NIMG // 2
    half = math.pi / NIMG
    phase = ((k * (2 * start + length - 1)) & (2 * NIMG - 1)).astype(F32) * half
    top = jnp.sin(((k * length) & (2 * NIMG - 1)).astype(F32) * half)
    bottom = jnp.sin(k.astype(F32) * half)
    zero = k == 0
    ratio = jnp.where(zero, float(length), top / jnp.where(zero, 1.0, bottom))
    phase = jnp.where(zero, 0.0, phase)
    return ratio * jnp.cos(phase), ratio * jnp.sin(phase)


def mm(a, b):
    return jnp.dot(a, b, preferred_element_type=F32)


def peers(n, ns):
    me = lax.axis_index("facet")
    z = lax.axis_index("sub")
    core = lax.rem(me, 2)
    chip = me // 2
    partner = me + 1 - 2 * core
    others = [lax.rem(chip + d, n // 2) * 2 + core for d in range(1, n // 2)]
    sources = [lax.rem(chip - d + n // 2, n // 2) * 2 + core for d in range(1, n // 2)]
    columns = [lax.rem(z + d, ns) for d in range(1, ns)]
    return me, z, core, chip, partner, others, sources, columns


def greet(partner, others, columns):
    barrier = pltpu.get_barrier_semaphore()
    for facet in [partner] + others:
        pl.semaphore_signal(barrier, inc=1, device_id={"facet": facet}, device_id_type=MESH)
    for column in columns:
        pl.semaphore_signal(barrier, inc=1, device_id={"sub": column}, device_id_type=MESH)


def send(src, dst, send_sem, recv_sem, **where):
    return pltpu.make_async_remote_copy(
        src_ref=src,
        dst_ref=dst,
        send_sem=send_sem,
        recv_sem=recv_sem,
        device_id=where,
        device_id_type=MESH,
    )


def step_kernel(
    n, ns, steps_ref, facet_ref, col_ref, row_ref, count_ref, model_ref, pos_ref, obs_ref, wt_ref,
    out_ref, res_ref,
    mb, table, s_ref, st, got_y, o_ref, offs, z_t, gacc, grid_t, ku_t, kv_t, acc, part_p, part_o,
    near_buf, send_buf, far_buf, adj, lag_t, tw_t, image_t, turned,
    ms, s1, r1, s2, r2, s3, r3, ss1, rs1, ss2, rs2, sl, sr, rz,
):
    rows, width = out_ref.shape
    blocks = width // STEP
    slots = pos_ref.shape[-1]
    half = n // 2
    norm = 1.0 / math.sqrt(n * rows * width)
    me, z, core, chip, partner, others, sources, columns = peers(n, ns)
    partner_core = 1 - core
    pixel = facet_ref[1, me]
    own = col_ref[0]
    greet(partner, others, columns)

    loads = []
    for j in range(blocks):
        where = pl.ds(j * STEP, STEP)
        load = pltpu.make_async_copy(model_ref.at[:, where], out_ref.at[:, where], ms.at[j])
        load.start()
        loads.append(load)
    o_ref[...] = jnp.full(o_ref.shape, own, jnp.int32)

    fine = 32
    q = iota((fine, SGW), 1) + own
    bc, bs = cis(q, pixel + fine * iota((STEP // fine, SGW), 0))
    cc, cs = cis(q, iota((fine, SGW), 0))
    for h in range(STEP // fine):
        hc, hs = bc[h : h + 1], bs[h : h + 1]
        table[h * fine : (h + 1) * fine, :SGW] = (hc * cc - hs * cs).astype(BF16)
        table[h * fine : (h + 1) * fine, SGW:] = (-(hc * cs + hs * cc)).astype(BF16)
    tc, ts = cis(iota((blocks, SGW), 1) + own, STEP * iota((blocks, SGW), 0))
    for j in range(blocks):
        loads[j].wait()
        mb[j * rows : (j + 1) * rows, :] = out_ref[:, j * STEP : (j + 1) * STEP].astype(BF16)
    yr = jnp.zeros((rows, SGW), F32)
    yi = jnp.zeros((rows, SGW), F32)
    group = max(blocks // 2, 1)
    for first in range(0, blocks, group):
        part = mm(mb[first * rows : (first + group) * rows, :], table[...])
        for j in range(group):
            pr, pi = part[j * rows : (j + 1) * rows, :SGW], part[j * rows : (j + 1) * rows, SGW:]
            c, s = tc[first + j : first + j + 1], ts[first + j : first + j + 1]
            yr += pr * c + pi * s
            yi += pi * c - pr * s
    s_ref[:, :SGW] = yr
    s_ref[:, SGW:] = yi
    st[0, :SGW, :] = yr.T.astype(BF16)
    st[0, SGW:, :] = yi.T.astype(BF16)
    pl.semaphore_wait(pltpu.get_barrier_semaphore(), 1 + len(others) + len(columns))

    def subgrid_tables():
        row_fine = 16
        q = iota((row_fine, SGW), 1) + row_ref[0, me]
        cc, cs = cis(q, iota((row_fine, SGW), 0))
        for f in range(n):
            steps = rows // row_fine
            bc, bs = cis(
                iota((steps, SGW), 1) + row_ref[0, me], facet_ref[0, f] + row_fine * iota((steps, SGW), 0)
            )
            for h in range(steps):
                hc, hs = bc[h : h + 1], bs[h : h + 1]
                at = h * row_fine
                z_t[f, at : at + row_fine, :] = (hc * cc - hs * cs).astype(BF16)
                z_t[f, rows + at : rows + at + row_fine, :] = (hc * cs + hs * cc).astype(BF16)
        cells = iota((SGW, VB), 0).astype(F32) + 0.5

        def kernel_of(position):
            distance = cells - position.astype(F32) * (1.0 / OS)
            square = distance * distance
            return jnp.where(square <= float(KSUP * KSUP), jnp.exp(-0.5 * square), 0.0).astype(BF16)

        def block(i, carry):
            part = pl.ds(pl.multiple_of(i * VB, VB), VB)
            ku_t[:, part] = kernel_of(pos_ref[0, 0, 0:1, part])
            kv_t[:, part] = kernel_of(pos_ref[1, 0, 0:1, part])
            return carry

        lax.fori_loop(0, slots // VB, block, 0)

    def lag_tables(first, stop):
        lags = iota((1, 2 * SGW), 1)
        lags = jnp.where(lags < SGW, lags, lags - 2 * SGW)

        def column(c, carry):
            other = jnp.broadcast_to(offs[c][0:1, 0:1], (1, 2 * SGW))
            d1 = dirichlet(other - own - lags, pixel, width)
            d2 = dirichlet(-(other + own + SGW - 1 + lags), pixel, width)
            for i, line in enumerate(d1 + d2):
                wide = jnp.broadcast_to(line, (SGW, 2 * SGW))
                lag_t[c, i] = pltpu.roll(wide, 0, 1, stride=1, stride_axis=0)[:, :SGW].astype(BF16)
            return carry

        lax.fori_loop(first, stop, column, 0)

    def image_tables(first, stop):
        lane_fine = 128
        coarse = STEP // lane_fine

        def column(c, carry):
            other = offs[c][0:1, 0:1]
            tc, ts = cis(iota((blocks, SGW), 1) + other, STEP * iota((blocks, SGW), 0))
            tw_t[c, :, :SGW] = tc
            tw_t[c, :, SGW:] = ts
            q = iota((SGW, lane_fine), 0) + other
            bc, bs = cis(q, pixel + lane_fine * iota((SGW, lane_fine), 1))
            cc, cs = cis(q, iota((SGW, lane_fine), 1))
            for h in range(coarse):
                hc, hs = bc[:, h : h + 1], bs[:, h : h + 1]
                part = slice(h * lane_fine, (h + 1) * lane_fine)
                image_t[c, :SGW, part] = (hc * cc - hs * cs).astype(BF16)
                image_t[c, SGW:, part] = (-(hc * cs + hs * cc)).astype(BF16)
            return carry

        lax.fori_loop(first, stop, column, 0)

    def grid_term(t, f):
        yr, yi = got_y[t, f, :SGW, :], got_y[t, f, SGW:, :]
        zf = z_t[f]
        gacc[:SGW] += mm(jnp.concatenate([yr, yi], axis=1), zf)
        gacc[SGW:] += mm(jnp.concatenate([yi, -yr], axis=1), zf)

    def gather_sections(t, meanwhile):
        sent = []
        for d, other in enumerate(others):
            copy = send(st.at[t], got_y.at[t, me], s1.at[t, d + 1], r1.at[t, d + 1], facet=other)
            copy.start()
            sent.append(copy)
        near = send(st.at[t], got_y.at[t, me], s1.at[t, 0], r1.at[t, 0], facet=partner)
        near.start()
        sent.append(near)
        small = []
        if t == 0:
            for d, column in enumerate(columns):
                copy = send(o_ref, offs.at[z], s3.at[d], r3.at[d], sub=column)
                copy.start()
                sent.append(copy)
            offs[z] = o_ref[...]
        got_y[t, me] = st[t]
        meanwhile()
        gacc[...] = jnp.zeros_like(gacc)
        grid_term(t, me)
        send(st.at[t], got_y.at[t, partner], s1.at[t, 0], r1.at[t, 0], facet=partner).wait_recv()
        grid_term(t, partner)
        for d, source in enumerate(sources):
            send(st.at[t], got_y.at[t, source], s1.at[t, d + 1], r1.at[t, d + 1], facet=others[d]).wait_recv()
            block = got_y.at[t, source]
            copy = send(block, block, s2.at[t, d], r2.at[t, d], facet=partner)
            copy.start()
            sent.append(copy)
            grid_term(t, source)
        for d, source in enumerate(sources):
            twin = source - core + partner_core
            block = got_y.at[t, twin]
            send(block, block, s2.at[t, d], r2.at[t, d], facet=partner).wait_recv()
            grid_term(t, twin)
        for copy in sent:
            copy.wait_send()
        grid_t[...] = (norm * gacc[...]).astype(BF16)

    def sweep(last):
        acc[...] = jnp.zeros_like(acc)
        lanes = iota((1, VB), 1)
        count = count_ref[0, me]

        def block(i, carry):
            start = pl.multiple_of(i * VB, VB)
            part = pl.ds(start, VB)
            ku = ku_t[:, part]
            kv = kv_t[:, part].astype(F32)
            h = mm(grid_t[...], ku)
            pr = jnp.sum(h[:SGW] * kv, axis=0, keepdims=True)
            pi = jnp.sum(h[SGW:] * kv, axis=0, keepdims=True)
            live = lanes + start < count
            weight = wt_ref[0, 0:1, part].astype(F32)
            rr = jnp.where(live, weight * (obs_ref[0, 0, 0:1, part].astype(F32) - pr), 0.0)
            ri = jnp.where(live, weight * (obs_ref[0, 0, 1:2, part].astype(F32) - pi), 0.0)
            if last:
                res_ref[0, 0, 0:1, part] = rr
                res_ref[1, 0, 0:1, part] = ri
            weighted = jnp.concatenate([(rr * kv).astype(BF16), (ri * kv).astype(BF16)], axis=0)
            acc[...] += lax.dot_general(ku, weighted, (((1,), (1,)), ((), ())), preferred_element_type=F32)
            return carry

        lax.fori_loop(0, slots // VB, block, 0)

    def exchange(t, meanwhile, use_column):
        gridded = acc[...].astype(BF16)

        def fold(dest):
            back = mm(z_t[dest], gridded)
            return back[:rows, :SGW] - back[rows:, SGW:], back[:rows, SGW:] + back[rows:, :SGW]

        order = list(range(1, half)) + [0]
        near = {}
        for d in order:
            real, imag = fold(lax.rem(chip + d, half) * 2 + partner_core)
            part_p[t, d, :, :SGW] = real.astype(BF16)
            part_p[t, d, :, SGW:] = imag.astype(BF16)
            near[d] = send(part_p.at[t, d], near_buf.at[t, d], ss1.at[t, d], rs1.at[t, d], facet=partner)
            near[d].start()
        for d in order:
            real, imag = fold(lax.rem(chip + d, half) * 2 + core)
            part_o[d, :, :SGW] = real
            part_o[d, :, SGW:] = imag
        size = rows // CHUNKS

        def away(d, k):
            cut = pl.ds(k * size, size)
            dest = lax.rem(chip + d, half) * 2 + core
            return send(
                send_buf.at[t, d, cut], far_buf.at[t, d, cut], ss2.at[t, d, k], rs2.at[t, d, k], facet=dest
            )

        for k in range(CHUNKS):
            cut = slice(k * size, (k + 1) * size)
            for d in range(1, half):
                if k == 0:
                    near[d].wait_recv()
                send_buf[t, d, cut] = (part_o[d, cut] + near_buf[t, d, cut].astype(F32)).astype(BF16)
                away(d, k).start()
        meanwhile()
        near[0].wait_recv()
        def hop(source, k, right):
            piece = adj.at[t, source, pl.ds(k * size, size)]
            sem = sr if right else sl
            to = z + 1 if right else z - 1
            return send(piece, piece, sem.at[t, source, k], rz.at[t, source, k], sub=to)

        for k in range(CHUNKS):
            cut = slice(k * size, (k + 1) * size)
            total = part_o[0, cut] + near_buf[t, 0, cut].astype(F32)
            for d in range(1, half):
                away(d, k).wait_recv()
                total += far_buf[t, d, cut].astype(F32)
            adj[t, z, cut] = total.astype(BF16)

            @pl.when(z < ns - 1)
            def _():
                hop(z, k, True).start()

            @pl.when(z > 0)
            def _():
                hop(z, k, False).start()

        use_column(z)
        for d in range(1, ns):
            for k in range(CHUNKS):

                @pl.when(z - d >= 0)
                def _():
                    hop(z - d, k, True).wait_recv()

                    @pl.when(z < ns - 1)
                    def _():
                        hop(z - d, k, True).start()

                @pl.when(z + d < ns)
                def _():
                    hop(z + d, k, False).wait_recv()

                    @pl.when(z > 0)
                    def _():
                        hop(z + d, k, False).start()

            @pl.when(z - d >= 0)
            def _():
                use_column(z - d)

            @pl.when(z + d < ns)
            def _():
                use_column(z + d)

        for copy in near.values():
            copy.wait_send()
        for d in range(1, half):
            for k in range(CHUNKS):
                away(d, k).wait_send()
        for d in range(0, ns):
            for k in range(CHUNKS):

                @pl.when((z - d >= 0) & (z < ns - 1))
                def _():
                    hop(z - d, k, True).wait_send()

                @pl.when((z + d < ns) & (z > 0))
                def _():
                    hop(z + d, k, False).wait_send()

    mirror = (iota((SGW, SGW), 0) + iota((SGW, SGW), 1) == SGW - 1).astype(F32).astype(BF16)

    def add_to_section(c):
        scale = steps_ref[0] * (0.5 * norm)
        ar, ai = adj[0, c, :, :SGW], adj[0, c, :, SGW:]
        vr, vi = mm(ar, mirror).astype(BF16), mm(ai, mirror).astype(BF16)
        d1r, d1i, d2r, d2i = lag_t[c, 0], lag_t[c, 1], lag_t[c, 2], lag_t[c, 3]
        s_ref[:, :SGW] += scale * (mm(ar, d1r) - mm(ai, d1i) + mm(vr, d2r) + mm(vi, d2i))
        s_ref[:, SGW:] += scale * (mm(ar, d1i) + mm(ai, d1r) + mm(vr, d2i) - mm(vi, d2r))

    def add_to_image(c):
        a = (steps_ref[0] * norm) * adj[0, c].astype(F32) + (steps_ref[1] * norm) * adj[1, c].astype(F32)
        ar, ai = a[:, :SGW], a[:, SGW:]
        for j in range(blocks):
            tc, ts = tw_t[c, j : j + 1, :SGW], tw_t[c, j : j + 1, SGW:]
            turned[j * rows : (j + 1) * rows, :SGW] = (ar * tc - ai * ts).astype(BF16)
            turned[j * rows : (j + 1) * rows, SGW:] = (ar * ts + ai * tc).astype(BF16)
        lanes = 256

        def chunk(i, carry):
            got = mm(turned[...], image_t[c, :, pl.ds(pl.multiple_of(i * lanes, lanes), lanes)])
            for j in range(blocks):
                where = pl.ds(pl.multiple_of(j * STEP + i * lanes, lanes), lanes)
                out_ref[:, where] += got[j * rows : (j + 1) * rows]
            return carry

        lax.fori_loop(0, STEP // lanes, chunk, 0)

    def first_tables():
        subgrid_tables()
        for d in range(ns - 1):
            source = lax.rem(z - d - 1 + ns, ns)
            send(o_ref, offs.at[source], s3.at[d], r3.at[d], sub=columns[d]).wait_recv()
        lag_tables(0, ns // 2)

    gather_sections(0, first_tables)
    sweep(False)
    exchange(0, lambda: lag_tables(ns // 2, ns), add_to_section)
    st[1, :SGW, :] = s_ref[:, :SGW].T.astype(BF16)
    st[1, SGW:, :] = s_ref[:, SGW:].T.astype(BF16)
    gather_sections(1, lambda: image_tables(0, ns // 2))
    sweep(True)
    exchange(1, lambda: image_tables(ns // 2, ns), add_to_image)


def local(model_image, step_sizes, facet_offsets, col_offsets, row_offsets, counts, vis_uv, vis_obs, vis_weight):
    n = lax.axis_size("facet")
    ns = lax.axis_size("sub")
    model = model_image[0]
    rows, width = model.shape
    slots = vis_uv.shape[-1]
    half = n // 2
    blocks = width // STEP
    dma = pltpu.SemaphoreType.DMA
    vmem = pl.BlockSpec(memory_space=VMEM)
    smem = pl.BlockSpec(memory_space=pltpu.SMEM)
    observed = jnp.transpose(vis_obs, (1, 2, 0, 3))
    buffers = [
            VMEM((blocks * rows, STEP), BF16),
            VMEM((STEP, 2 * SGW), BF16),
            VMEM((rows, 2 * SGW), F32),
            VMEM((ITERS, 2 * SGW, rows), BF16),
            VMEM((ITERS, n, 2 * SGW, rows), BF16),
            VMEM((8, 128), jnp.int32),
            VMEM((ns, 8, 128), jnp.int32),
            VMEM((n, 2 * rows, SGW), BF16),
            VMEM((2 * SGW, SGW), F32),
            VMEM((2 * SGW, SGW), BF16),
            VMEM((SGW, slots), BF16),
            VMEM((SGW, slots), BF16),
            VMEM((SGW, 2 * SGW), F32),
            VMEM((ITERS, half, rows, 2 * SGW), BF16),
            VMEM((half, rows, 2 * SGW), F32),
            VMEM((ITERS, half, rows, 2 * SGW), BF16),
            VMEM((ITERS, half, rows, 2 * SGW), BF16),
            VMEM((ITERS, half, rows, 2 * SGW), BF16),
            VMEM((ITERS, ns, rows, 2 * SGW), BF16),
            VMEM((ns, 4, SGW, SGW), BF16),
            VMEM((ns, blocks, 2 * SGW), F32),
            VMEM((ns, 2 * SGW, STEP), BF16),
            VMEM((blocks * rows, 2 * SGW), BF16),
    ]
    kept = 4 * (rows * width + 2 * slots) + 2**17
    image, residual = pl.pallas_call(
        functools.partial(step_kernel, n, ns),
        out_shape=(
            VMEM(model.shape, F32),
            VMEM((2, 1, 1, slots), F32),
        ),
        in_specs=[smem] * 5 + [pl.BlockSpec(memory_space=pl.ANY)] + [vmem] * 3,
        out_specs=(vmem, vmem),
        scratch_shapes=buffers
        + [
            dma((blocks,)),
            dma((ITERS, half)),
            dma((ITERS, half)),
            dma((ITERS, half)),
            dma((ITERS, half)),
            dma((ns,)),
            dma((ns,)),
            dma((ITERS, half)),
            dma((ITERS, half)),
            dma((ITERS, half, CHUNKS)),
            dma((ITERS, half, CHUNKS)),
            dma((ITERS, ns, CHUNKS)),
            dma((ITERS, ns, CHUNKS)),
            dma((ITERS, ns, CHUNKS)),
        ],
        compiler_params=pltpu.CompilerParams(
            collective_id=0, has_side_effects=True, vmem_limit_bytes=VMEM_BYTES - kept
        ),
        name="cycles",
    )(step_sizes, facet_offsets, col_offsets, row_offsets, counts, model, vis_uv, observed, vis_weight)
    return (image[None], residual)


def solution(mesh):
    in_specs = (
        P("facet", None, None),
        P(),
        P(),
        P("sub"),
        P("sub", None),
        P("sub", None),
        P(None, "sub", "facet", None),
        P(None, "sub", "facet", None),
        P("sub", "facet", None),
    )
    out_specs = (P("facet", None, None), P(None, "sub", "facet", None))
    return jax.shard_map(local, mesh=mesh, in_specs=in_specs, out_specs=out_specs, check_vma=False)
```
